512 devices in a mesh: parts: 2 (over y), expert: 64 (over z, core), tensor: 4 (over x).
Axes of the slice: x: 4, y: 2, z: 32, core: 2. Of those that a mesh axis runs over, the one named last changes fastest.
The devices are a block of a 4x8x32 slice.
Arguments:
- tokens: bfloat16 [2048, 6144], P(('parts', 'expert'), 'tensor'), parts along dimension 0, may hold values from -4 to 4
- queries: bfloat16 [2048, 48, 128], P(('parts', 'expert'), 'tensor'), parts along dimension 0, may hold values from -6 to 6
- new_kv: bfloat16 [2, 2048, 8, 128], P(None, ('parts', 'expert'), 'tensor'), parts along dimension 1, may hold values from -6 to 6
- cache_kv: bfloat16 [2, 2048, 16, 8, 128], P(None, ('parts', 'expert'), None, 'tensor'), parts along dimension 1, may hold values from -6 to 6
- lengths: int32 [2048], P(('parts', 'expert')), parts along dimension 0, may hold values from 2 to 16
- gain: float32 [6144], P('tensor'), may hold values from 0.1 to 1.9
- gate_weight: bfloat16 [6144, 32768], P('tensor', 'expert'), may hold values from -0.078125 to 0.078125
- up_weight: bfloat16 [6144, 32768], P('tensor', 'expert'), may hold values from -0.078125 to 0.078125
- down_weight: bfloat16 [32768, 6144], P('expert', 'tensor'), may hold values from -0.0625 to 0.0625
- routes: int32 [2048, 2], P(('parts', 'expert')), parts along dimension 0, may hold values from 0 to 3, all different within a row; in each aligned block of 16 rows (0 to 15, 16 to 31, ...) at most 9 rows name the same one
- route_weights: bfloat16 [2048, 2], P(('parts', 'expert')), parts along dimension 0, may hold values from 0.19921875 to 0.796875
Outputs:
- mixed: bfloat16 [2048, 6144], P(('parts', 'expert'), 'tensor'), parts along dimension 0
The draws below stay inside these ranges and needn't reach their ends.
There are 2 independent parts, one for each index of `parts`. The reference program is written for one: setup_inputs(seed, part) draws one part's arguments, and reference() takes and returns one part's arrays. A program takes and returns all parts, laid end to end along the dimension named above; an argument that names none is the same for every part. Nothing has to cross between parts.
Inputs may be any that keep to these rules, and one draw needn't show every extreme that they name: `routes`: the two entries of a row differ; in the rows of one index of expert no expert is named more than 9 times, a bound that some block reaches there in every draw.
All inputs are finite; a program needn't handle non-finite values.
Results may differ from the reference program's by a relative error of at most 0.0094.
Values may be sent and summed in bfloat16 or wider, within the bound.
No kernel may reach another device: no remote copies, remote signals or barrier semaphores. Data moves between devices by JAX's collectives and lax.ppermute only.
A program may use at most 64 MiB of HBM per device.

```python
import math
import jax
import jax.numpy as jnp
import numpy as np
from jax import lax

D = 6144
QH = 48
KVH = 8
HD = 128
EXPERTS = 4
FF = 8192
CTX = 16
SEQ_DEV = 16
CAP = 9
TOKENS = 1024


def draw_tokens(key, part):
    folded = jax.random.fold_in(key, 11)
    key_entries, key_rough, key_rows = jax.random.split(folded, 3)
    rising = jnp.exp(math.log(3.0) * jnp.arange(D, dtype=jnp.float32) / D)
    roughness = jnp.exp(jax.random.uniform(key_rough, (D,), jnp.float32, math.log(0.6), math.log(1.8)))
    columns = rising * roughness
    entries = jnp.clip(jax.random.normal(key_entries, (TOKENS, D), jnp.float32), -3.0, 3.0)
    scales = jnp.exp(jax.random.uniform(key_rows, (TOKENS, 1), jnp.float32, math.log(0.05), math.log(0.5)))
    return jnp.clip(entries * scales * columns, -4.0, 4.0).astype(jnp.bfloat16)


def draw_queries(key, part):
    key_query = jax.random.fold_in(key, 21)
    return jnp.clip(jax.random.normal(key_query, (TOKENS, QH, HD), jnp.float32), -6.0, 6.0).astype(jnp.bfloat16)


def draw_cache_kv(key, part):
    key_cache = jax.random.fold_in(key, 33)
    return jnp.clip(jax.random.normal(key_cache, (2, TOKENS, CTX, KVH, HD), jnp.float32), -6.0, 6.0).astype(jnp.bfloat16)


def set_ends(array, key, least, high):
    index_at = [jax.random.randint(jax.random.fold_in(key, axis), (), 0, length) for axis, length in enumerate(array.shape)]
    main_axis = array.shape.index(max(array.shape))
    beside = index_at[:main_axis] + [(index_at[main_axis] + 1) % array.shape[main_axis]] + index_at[main_axis + 1:]
    return array.at[tuple(index_at)].set(least).at[tuple(beside)].set(high)


def steps_of(key, extent, pieces, low, high):
    loudness, own = 1.0, jax.random.fold_in(key, 6)
    for dim, parts in pieces:
        draws = jnp.exp(jax.random.uniform(jax.random.fold_in(own, dim), (parts,), jnp.float32, low / len(pieces), high / len(pieces)))
        loudness = loudness * jnp.repeat(draws, extent[dim] // parts).reshape([-1 if axis == dim else 1 for axis in range(len(extent))])
    return loudness


def assign_block(key, own, number, rows, number_of, top, most, lean):
    order = jax.random.permutation(key, number_of)
    packed, common = load_shares(number_of, rows * top, most, lean, True), load_shares(number_of, rows * top, most, lean, False)
    places = jnp.arange(number_of)

    def named(sizes, turn):
        used = int((sizes > 0).sum())
        fixed = max(1, used // 4)
        moved = fixed + (places - fixed + turn * (used - fixed)) % max(1, number_of - fixed)
        return jnp.zeros((number_of,), jnp.int32).at[order[jnp.where(places < fixed, places, moved)]].set(jnp.asarray(sizes, jnp.int32))

    sizes = jnp.where(number % 4 == 0, named(packed, number // 4), named(common, number - number // 4 - 1))
    mixed = jax.random.permutation(jax.random.fold_in(own, 3), number_of)
    giver, receiver = mixed[0:number_of // 2 * 2:2], mixed[1:number_of // 2 * 2:2]
    margin = jnp.minimum(sizes[giver] - 1, most - sizes[receiver]) // 2
    margin = jnp.where((giver == order[0]) | (receiver == order[0]) | (sizes[receiver] == 0), 0, jnp.maximum(margin, 0))
    moved = jax.random.randint(jax.random.fold_in(own, 4), (number_of // 2,), 0, 1 << 20) % (margin + 1)
    sizes = sizes.at[giver].add(-moved).at[receiver].add(moved)
    items = jnp.searchsorted(jnp.cumsum(sizes), jnp.arange(rows * top), side="right").astype(jnp.int32)
    table = items.reshape(top, rows).T
    table = table[jax.random.permutation(jax.random.fold_in(own, 1), rows)]
    turn = jax.random.randint(jax.random.fold_in(own, 2), (rows, 1), 0, top)
    return jnp.take_along_axis(table, (jnp.arange(top)[None, :] + turn) % top, axis=1)


def load_shares(count, total, reach, lean, full):
    portions = [(1 << 20) // math.isqrt(grade ** lean) + 1 for grade in range(1, count + 1)]
    largest = reach if full else min(reach, max(-(-total // count), total * portions[0] // sum(portions)))
    least = 1 if total - largest >= count - 1 else 0
    counts, rest = [largest] + [least] * (count - 1), total - largest - least * (count - 1)
    while rest > 0:
        candidates = [i for i in range(1, count) if counts[i] < largest] or [i for i in range(1, count) if counts[i] < reach]
        pool, left = sum([portions[i] for i in candidates]), rest
        for i in candidates:
            addition = min(reach - counts[i], max(1, left * portions[i] // pool), rest)
            counts[i] = counts[i] + addition
            rest = rest - addition
    return np.array(counts)


def scatter_about(own_key, dims, scale, bound, shards=(), kind=jnp.bfloat16):
    loudness = steps_of(own_key, dims, shards, -0.22, 0.18) if shards else 1.0
    values = jax.random.normal(own_key, dims, jnp.float32) * scale * loudness
    return jnp.minimum(jnp.maximum(values, -bound), bound).astype(kind)


def setup_inputs(seed: int = 0, part: int = 0) -> dict:
    key_of = jax.random.split(jax.random.key(seed), 12)
    part_keys = jax.random.split(jax.random.fold_in(key_of[11], part), 12)
    tokens = draw_tokens(jax.random.fold_in(jax.random.fold_in(key_of[11], part), 71), part)
    queries = draw_queries(jax.random.fold_in(jax.random.fold_in(key_of[11], part), 71), part)
    new_kv = scatter_about(part_keys[2], (2, TOKENS, KVH, HD), 1.0, 6.0, ((1, 64), (2, 4)))
    cache_kv = draw_cache_kv(jax.random.fold_in(jax.random.fold_in(key_of[11], part), 71), part)
    lengths = set_ends(jax.random.randint(part_keys[4], (TOKENS,), 2, CTX + 1), jax.random.fold_in(part_keys[4], 1), 2, CTX).astype(jnp.int32)
    gain = jnp.clip(1.0 + 0.18 * jax.random.normal(key_of[5], (D,), jnp.float32), 0.1, 1.9)
    gate_weight = scatter_about(key_of[6], (D, EXPERTS * FF), D ** -0.5, 0.078125, ((0, 4), (1, 64)))
    up_weight = scatter_about(key_of[7], (D, EXPERTS * FF), D ** -0.5, 0.078125, ((0, 4), (1, 64)))
    down_weight = scatter_about(key_of[8], (EXPERTS * FF, D), FF ** -0.5, 0.0625, ((0, 64), (1, 4)))
    routes_keys = jax.random.split(jax.random.fold_in(part_keys[9], 1), TOKENS // SEQ_DEV)
    routes_turns = jax.random.permutation(jax.random.fold_in(part_keys[9], 3), TOKENS // SEQ_DEV)
    routes = jax.vmap(lambda own, number: assign_block(jax.random.fold_in(part_keys[9], 2), own, number, SEQ_DEV, EXPERTS, 2, CAP, 2))(routes_keys, routes_turns).reshape((TOKENS, 2))
    route_weights = jnp.clip(0.19921875 + 0.59765625 * jax.random.uniform(part_keys[10], (TOKENS, 2), jnp.float32) ** steps_of(part_keys[10], (TOKENS, 2), ((0, 64),), -0.2, 0.2), 0.19921875, 0.796875).astype(jnp.bfloat16)
    return {"tokens": tokens, "queries": queries, "new_kv": new_kv, "cache_kv": cache_kv, "lengths": lengths, "gain": gain, "gate_weight": gate_weight, "up_weight": up_weight, "down_weight": down_weight, "routes": routes, "route_weights": route_weights}


EPSILON = 1e-05

def attend(queries, new_kv, cache_kv, lengths):
    groups = QH // KVH
    sequences = queries.shape[0]
    factor = 1.0 / math.sqrt(HD)
    query_grp = queries.astype(jnp.float32).reshape(sequences, KVH, groups, HD)
    key_old = cache_kv[0].astype(jnp.float32)
    value_old = cache_kv[1].astype(jnp.float32)
    key_new = new_kv[0].astype(jnp.float32)
    value_new = new_kv[1].astype(jnp.float32)
    score_old = jnp.einsum('skgd,spkd->skgp', query_grp, key_old) * factor
    score_new = jnp.einsum('skgd,skd->skg', query_grp, key_new) * factor
    position = jnp.arange(key_old.shape[1], dtype=jnp.int32)
    usable = (position[None, :] < lengths[:, None])[:, None, None, :]
    score_old = jnp.where(usable, score_old, -jnp.inf)
    largest = jnp.maximum(lax.optimization_barrier(jnp.max(score_old, axis=3)), score_new)
    weight_old = jnp.exp(score_old - largest[..., None])
    weight_new = jnp.exp(score_new - largest)
    denominator = lax.optimization_barrier(jnp.sum(weight_old, axis=3)) + weight_new
    prob_old = lax.optimization_barrier((weight_old / denominator[..., None]).astype(jnp.bfloat16))
    prob_new = lax.optimization_barrier((weight_new / denominator).astype(jnp.bfloat16))
    attended = jnp.einsum('skgp,spkd->skgd', prob_old.astype(jnp.float32), value_old)
    attended = attended + prob_new.astype(jnp.float32)[..., None] * value_new[:, :, None, :]
    return attended.reshape(sequences, KVH * groups * HD)

def reference(tokens, queries, new_kv, cache_kv, lengths, gain, gate_weight, up_weight, down_weight, routes, route_weights):
    residual = tokens.astype(jnp.float32) + attend(queries, new_kv, cache_kv, lengths)
    row_ss = lax.optimization_barrier(jnp.sum(residual * residual, axis=1))
    normed = (residual * lax.rsqrt(row_ss[:, None] / D + EPSILON) * gain).astype(jnp.bfloat16)
    moe_sum = jnp.zeros(residual.shape, jnp.float32)
    for expert in range(EXPERTS):
        first = expert * FF
        gate_sum = jnp.dot(normed, gate_weight[:, first:first + FF], preferred_element_type=jnp.float32)
        lift_sum = jnp.dot(normed, up_weight[:, first:first + FF], preferred_element_type=jnp.float32)
        hidden = (jax.nn.silu(gate_sum) * lift_sum).astype(jnp.bfloat16)
        produced = jnp.dot(hidden, down_weight[first:first + FF, :], preferred_element_type=jnp.float32)
        share = lax.optimization_barrier(jnp.sum(jnp.where(routes == expert, route_weights.astype(jnp.float32), jnp.float32(0.0)), axis=1))
        moe_sum = moe_sum + share[:, None] * produced
    return (residual + moe_sum).astype(jnp.bfloat16)
```

```python
import math

import jax
import jax.numpy as jnp
from jax import lax
from jax.sharding import Mesh
from jax.sharding import PartitionSpec as P

EXPERTS = 4
CAP = 9
EXPERT = ("seg", "pos", "core")
PARTS_EXPERT = ("parts", "seg", "pos", "core")
LANES = 128

EPSILON = 1e-05


def shifted(x, axis, by):
    count = lax.axis_size(axis)
    return lax.ppermute(x, axis, [(i, (i + by) % count) for i in range(count)])


def from_partner(x, axis, apart):
    return lax.ppermute(x, axis, [(i, i ^ apart) for i in range(lax.axis_size(axis))])


def attend(queries, new_kv, cache_kv, lengths):
    sequences, head_count, head_size = queries.shape
    key_heads = new_kv.shape[2]
    groups = head_count // key_heads
    factor = 1.0 / math.sqrt(head_size)
    query_grp = queries.reshape(sequences, key_heads, groups, head_size)
    score_old = (
        jnp.einsum("skgd,spkd->skgp", query_grp, cache_kv[0], preferred_element_type=jnp.float32)
        * factor
    )
    score_new = (
        jnp.einsum("skgd,skd->skg", query_grp, new_kv[0], preferred_element_type=jnp.float32)
        * factor
    )
    position = jnp.arange(cache_kv.shape[2], dtype=jnp.int32)
    usable = (position[None, :] < lengths[:, None])[:, None, None, :]
    score_old = jnp.where(usable, score_old, -jnp.inf)
    largest = jnp.maximum(jnp.max(score_old, axis=3), score_new)
    weight_old = jnp.exp(score_old - largest[..., None])
    weight_new = jnp.exp(score_new - largest)
    denominator = jnp.sum(weight_old, axis=3) + weight_new
    prob_old = (weight_old / denominator[..., None]).astype(jnp.bfloat16)
    prob_new = (weight_new / denominator).astype(jnp.bfloat16)
    attended = jnp.einsum(
        "skgp,spkd->skgd", prob_old, cache_kv[1], preferred_element_type=jnp.float32
    )
    attended = (
        attended
        + prob_new.astype(jnp.float32)[..., None] * new_kv[1].astype(jnp.float32)[:, :, None, :]
    )
    return attended.reshape(sequences, head_count * head_size)


def doubled(rows, axis, apart):
    return jnp.concatenate([rows, from_partner(rows, axis, apart)], axis=0)


def halved(terms, axis, apart):
    half = terms.shape[0] // 2
    arrived = from_partner(terms[half:].astype(jnp.bfloat16), axis, apart)
    return terms[:half] + arrived.astype(jnp.float32)


def exchanged(blocks, back):
    sign = -1 if back else 1
    return jnp.stack(
        [blocks[0]] + [shifted(blocks[r], "seg", sign * r) for r in range(1, EXPERTS)]
    )


def expert_part(rows, gain, gate_weight, up_weight, down_weight):
    count, local_width = rows.shape
    columns = gate_weight.shape[1]
    across = lax.axis_size("tensor")
    plain = rows.astype(jnp.float32) / gain
    squares = jnp.sum(plain * plain, axis=1, keepdims=True)
    squares_high = lax.reduce_precision(squares, 8, 7)
    squares_low = squares - squares_high
    lane = lax.broadcasted_iota(jnp.int32, (count, LANES), 1)
    squares = jnp.where(lane == 0, squares_high, squares_low).astype(jnp.bfloat16)
    gate_sum = jnp.dot(rows, gate_weight, preferred_element_type=jnp.float32)
    lift_sum = jnp.dot(rows, up_weight, preferred_element_type=jnp.float32)
    sums = jnp.concatenate(
        [gate_sum.astype(jnp.bfloat16), lift_sum.astype(jnp.bfloat16), squares], axis=1
    )
    sums = sums.reshape(across, count // across, sums.shape[1])
    sums = lax.all_to_all(sums, "tensor", split_axis=0, concat_axis=0, tiled=True)
    sums = jnp.sum(sums.astype(jnp.float32), axis=0)
    squares = sums[:, 2 * columns : 2 * columns + 1] + sums[:, 2 * columns + 1 : 2 * columns + 2]
    scale = lax.rsqrt(squares / (local_width * across) + EPSILON)
    hidden = jax.nn.silu(sums[:, :columns] * scale) * (sums[:, columns : 2 * columns] * scale)
    hidden = hidden.astype(jnp.bfloat16)
    copies = jnp.broadcast_to(hidden, (across, *hidden.shape))
    hidden = lax.all_to_all(copies, "tensor", split_axis=0, concat_axis=0, tiled=True)
    hidden = hidden.reshape(count, columns)
    return jnp.dot(hidden, down_weight, preferred_element_type=jnp.float32)


def on_device(
    tokens,
    queries,
    new_kv,
    cache_kv,
    lengths,
    gain,
    gate_weight,
    up_weight,
    down_weight,
    routes,
    route_weights,
):
    local_seqs, local_width = tokens.shape
    residual = tokens.astype(jnp.float32) + attend(queries, new_kv, cache_kv, lengths)
    scaled = (residual * gain).astype(jnp.bfloat16)
    ahead = (routes - lax.axis_index("seg") + EXPERTS) % EXPERTS
    choosers = (ahead[:, :, None] == jnp.arange(EXPERTS, dtype=jnp.int32)[None, None, :]).astype(
        jnp.int32
    )
    flat_choice = choosers.reshape(2 * local_seqs, EXPERTS)
    earlier = jnp.cumsum(flat_choice, axis=0) - flat_choice
    slot_index = jnp.sum(earlier * flat_choice, axis=1)
    target = (ahead.reshape(-1) * CAP + slot_index).reshape(local_seqs, 2)
    slot_ids = jnp.arange(EXPERTS * CAP, dtype=jnp.int32)
    placing = jnp.sum(
        (slot_ids[:, None, None] == target[None, :, :]).astype(jnp.float32), axis=2
    ).astype(jnp.bfloat16)
    mixing = jnp.sum(
        jnp.where(
            slot_ids[None, None, :] == target[:, :, None],
            route_weights.astype(jnp.float32)[:, :, None],
            jnp.float32(0.0),
        ),
        axis=1,
    ).astype(jnp.bfloat16)
    packed = jnp.dot(placing, scaled, preferred_element_type=jnp.float32).astype(jnp.bfloat16)
    flat = (EXPERTS, CAP * local_width // LANES, LANES)
    rows = exchanged(packed.reshape(flat), False).reshape(EXPERTS * CAP, local_width)
    distances = [1 << bit for bit in range(lax.axis_size("pos").bit_length() - 1)]
    for apart in reversed(distances):
        rows = doubled(rows, "pos", apart)
    rows = doubled(rows, "core", 1)
    produced = expert_part(rows, gain, gate_weight, up_weight, down_weight)
    produced = halved(produced, "core", 1)
    for apart in distances:
        produced = halved(produced, "pos", apart)
    returned = exchanged(produced.astype(jnp.bfloat16).reshape(flat), True)
    per_slot = returned.reshape(EXPERTS * CAP, local_width)
    moe_sum = jnp.dot(mixing, per_slot, preferred_element_type=jnp.float32)
    return (residual + moe_sum).astype(jnp.bfloat16)


def solution(mesh):
    split = Mesh(
        mesh.devices.reshape(
            mesh.shape["parts"], EXPERTS, mesh.shape["expert"] // (2 * EXPERTS), 2, mesh.shape["tensor"]
        ),
        ("parts", "seg", "pos", "core", "tensor"),
    )
    return jax.shard_map(
        on_device,
        mesh=split,
        in_specs=(
            P(PARTS_EXPERT, "tensor"),
            P(PARTS_EXPERT, "tensor", None),
            P(None, PARTS_EXPERT, "tensor", None),
            P(None, PARTS_EXPERT, None, "tensor", None),
            P(PARTS_EXPERT),
            P("tensor"),
            P("tensor", EXPERT),
            P("tensor", EXPERT),
            P(EXPERT, "tensor"),
            P(PARTS_EXPERT, None),
            P(PARTS_EXPERT, None),
        ),
        out_specs=P(PARTS_EXPERT, "tensor"),
        check_vma=False,
    )
```

```python
import functools
import math

import jax
import jax.numpy as jnp
from jax import lax
from jax.experimental import pallas as pl
from jax.experimental.pallas import tpu as pltpu
from jax.sharding import Mesh
from jax.sharding import PartitionSpec as P


EXPERTS = 4
CAP = 9
EXPERT = ("seg", "pos", "core")
PARTS_EXPERT = ("parts", "seg", "pos", "core")
LANES = 128

EPSILON = 1e-05


def from_partner(x, axis, apart):
    return lax.ppermute(x, axis, [(i, i ^ apart) for i in range(lax.axis_size(axis))])


def attend(queries, new_kv, cache_kv, lengths):
    sequences, head_count, head_size = queries.shape
    key_heads = new_kv.shape[2]
    groups = head_count // key_heads
    factor = 1.0 / math.sqrt(head_size)
    query_grp = queries.reshape(sequences, key_heads, groups, head_size)
    score_old = (
        jnp.einsum("skgd,spkd->skgp", query_grp, cache_kv[0], preferred_element_type=jnp.float32)
        * factor
    )
    score_new = (
        jnp.einsum("skgd,skd->skg", query_grp, new_kv[0], preferred_element_type=jnp.float32)
        * factor
    )
    position = jnp.arange(cache_kv.shape[2], dtype=jnp.int32)
    usable = (position[None, :] < lengths[:, None])[:, None, None, :]
    score_old = jnp.where(usable, score_old, -jnp.inf)
    largest = jnp.maximum(jnp.max(score_old, axis=3), score_new)
    weight_old = jnp.exp(score_old - largest[..., None])
    weight_new = jnp.exp(score_new - largest)
    denominator = jnp.sum(weight_old, axis=3) + weight_new
    prob_old = (weight_old / denominator[..., None]).astype(jnp.bfloat16)
    prob_new = (weight_new / denominator).astype(jnp.bfloat16)
    attended = jnp.einsum(
        "skgp,spkd->skgd", prob_old, cache_kv[1], preferred_element_type=jnp.float32
    )
    attended = (
        attended
        + prob_new.astype(jnp.float32)[..., None] * new_kv[1].astype(jnp.float32)[:, :, None, :]
    )
    return attended.reshape(sequences, head_count * head_size)


def between_segments(blocks):
    segs, places, cores = (lax.axis_size(a) for a in EXPERT)
    groups = [
        [
            (seg * places + (place + places // 2 * (2 * seg // segs)) % places) * cores + core
            for seg in range(segs)
        ]
        for place in range(places)
        for core in range(cores)
    ]
    return lax.all_to_all(
        blocks, EXPERT, split_axis=0, concat_axis=0, tiled=True, axis_index_groups=groups
    )


def kept(x):
    return pltpu.with_memory_space_constraint(x, pltpu.VMEM)


def up_kernel(*refs):
    pieces, (gain_ref, gate_ref, up_ref, out_ref, rows_ref) = refs[:-5], refs[-5:]
    across, share, _ = out_ref.shape
    columns = gate_ref.shape[1]
    count = pieces[0].shape[0]
    inverse = 1.0 / gain_ref[...]
    lane = lax.broadcasted_iota(jnp.int32, (count, LANES), 1)
    for i, piece in enumerate(pieces):
        rows = piece[...]
        rows_ref[i * count : (i + 1) * count, :] = rows
        plain = rows.astype(jnp.float32) * inverse
        squares = jnp.sum(plain * plain, axis=1, keepdims=True)
        high = squares.astype(jnp.bfloat16).astype(jnp.float32)
        both = jnp.where(lane == 0, high, squares - high).astype(jnp.bfloat16)
        out_ref[i, :, 2 * columns :] = both
    for at, weight in ((0, gate_ref), (columns, up_ref)):
        sums = jnp.dot(rows_ref[...], weight[...], preferred_element_type=jnp.float32)
        sums = sums.astype(jnp.bfloat16)
        for i in range(across):
            out_ref[i, :, at : at + columns] = sums[i * share : (i + 1) * share]


def up_part(pieces, gain, gate_weight, up_weight):
    count, local_width = pieces[0].shape
    columns = gate_weight.shape[1]
    across = lax.axis_size("tensor")
    assert across == len(pieces)
    whole = pl.BlockSpec(memory_space=pltpu.VMEM)
    return pl.pallas_call(
        up_kernel,
        out_shape=pltpu.VMEM((across, count, 2 * columns + LANES), jnp.bfloat16),
        in_specs=[whole] * (len(pieces) + 3),
        out_specs=whole,
        scratch_shapes=[pltpu.VMEM((len(pieces) * count, local_width), jnp.bfloat16)],
        compiler_params=pltpu.CompilerParams(vmem_limit_bytes=16 << 20),
        name="up",
    )(*map(kept, (*pieces, gain.reshape(1, local_width), gate_weight, up_weight)))


def hidden_kernel(full_width, sums_ref, out_ref):
    across, _, width = sums_ref.shape
    columns = (width - LANES) // 2
    total = sums_ref[0].astype(jnp.float32)
    for i in range(1, across):
        total = total + sums_ref[i].astype(jnp.float32)
    squares = total[:, 2 * columns : 2 * columns + 1] + total[:, 2 * columns + 1 : 2 * columns + 2]
    scale = lax.rsqrt(squares / full_width + EPSILON)
    gate = total[:, :columns] * scale
    lift = total[:, columns : 2 * columns] * scale
    hidden = (gate / (1.0 + jnp.exp(-gate)) * lift).astype(jnp.bfloat16)
    for i in range(across):
        out_ref[i] = hidden


def activated(sums, full_width):
    across, count, width = sums.shape
    whole = pl.BlockSpec(memory_space=pltpu.VMEM)
    return pl.pallas_call(
        functools.partial(hidden_kernel, full_width),
        out_shape=pltpu.VMEM((across, count, (width - LANES) // 2), jnp.bfloat16),
        in_specs=[whole],
        out_specs=whole,
        compiler_params=pltpu.CompilerParams(vmem_limit_bytes=8 << 20),
        name="hidden",
    )(kept(sums))


def send(x):
    return x.astype(jnp.bfloat16)


def gathered(own):
    by4 = from_partner(own, "pos", 4)
    by2 = from_partner(own, "pos", 2)
    by6 = from_partner(by4, "pos", 2)
    near = jnp.concatenate([own, by4], axis=0)
    far = jnp.concatenate([by2, by6], axis=0)
    near_next = from_partner(near, "pos", 1)
    far_next = from_partner(far, "pos", 1)
    held = jnp.concatenate([near, far], axis=0)
    held_there = from_partner(held, "core", 1)
    following = jnp.concatenate([near_next, far_next], axis=0)
    following_there = from_partner(following, "core", 1)
    return held, following, held_there, following_there


def summed(terms):
    part = terms.shape[0] // 4
    held, following, held_there, following_there = (
        terms[i * part : (i + 1) * part] for i in range(4)
    )
    following = following + from_partner(send(following_there), "core", 1).astype(jnp.float32)
    held = held + from_partner(send(held_there), "core", 1).astype(jnp.float32)
    half = part // 2
    far = held[half:] + from_partner(send(following[half:]), "pos", 1).astype(jnp.float32)
    near = held[:half] + from_partner(send(following[:half]), "pos", 1).astype(jnp.float32)
    own = half // 2
    by4 = near[own:] + from_partner(send(far[own:]), "pos", 2).astype(jnp.float32)
    home = near[:own] + from_partner(send(far[:own]), "pos", 2).astype(jnp.float32)
    return home + from_partner(send(by4), "pos", 4).astype(jnp.float32)


def through_expert(pieces, gain, gate_weight, up_weight, down_weight):
    across = lax.axis_size("tensor")
    sums = up_part(pieces, gain, gate_weight, up_weight)
    sums = lax.all_to_all(sums, "tensor", split_axis=0, concat_axis=0, tiled=True)
    copies = activated(sums, gate_weight.shape[0] * across)
    hidden = lax.all_to_all(copies, "tensor", split_axis=0, concat_axis=0, tiled=True)
    hidden = hidden.reshape(-1, hidden.shape[2])
    return jnp.dot(hidden, down_weight, preferred_element_type=jnp.float32)


def on_device(
    tokens,
    queries,
    new_kv,
    cache_kv,
    lengths,
    gain,
    gate_weight,
    up_weight,
    down_weight,
    routes,
    route_weights,
):
    local_seqs, local_width = tokens.shape
    residual = tokens.astype(jnp.float32) + attend(queries, new_kv, cache_kv, lengths)
    scaled = (residual * gain).astype(jnp.bfloat16)
    choosers = (routes[:, :, None] == jnp.arange(EXPERTS, dtype=jnp.int32)[None, None, :]).astype(
        jnp.int32
    )
    flat_choice = choosers.reshape(2 * local_seqs, EXPERTS)
    earlier = jnp.cumsum(flat_choice, axis=0) - flat_choice
    slot_index = jnp.sum(earlier * flat_choice, axis=1)
    target = (routes.reshape(-1) * CAP + slot_index).reshape(local_seqs, 2)
    slot_ids = jnp.arange(EXPERTS * CAP, dtype=jnp.int32)
    placing = jnp.sum(
        (slot_ids[:, None, None] == target[None, :, :]).astype(jnp.float32), axis=2
    ).astype(jnp.bfloat16)
    mixing = jnp.sum(
        jnp.where(
            slot_ids[None, None, :] == target[:, :, None],
            route_weights.astype(jnp.float32)[:, :, None],
            jnp.float32(0.0),
        ),
        axis=1,
    ).astype(jnp.bfloat16)
    packed = jnp.dot(placing, scaled, preferred_element_type=jnp.float32).astype(jnp.bfloat16)
    flat = packed.reshape(EXPERTS, CAP * local_width // LANES, LANES)
    rows = between_segments(flat).reshape(EXPERTS * CAP, local_width)
    terms = through_expert(gathered(rows), gain, gate_weight, up_weight, down_weight)
    results = summed(terms).astype(jnp.bfloat16)
    results, mixing = lax.optimization_barrier((results, mixing))
    per_slot = between_segments(results.reshape(flat.shape)).reshape(EXPERTS * CAP, local_width)
    moe_sum = jnp.dot(mixing, per_slot, preferred_element_type=jnp.float32)
    return (residual + moe_sum).astype(jnp.bfloat16)


def solution(mesh):
    split = Mesh(
        mesh.devices.reshape(
            mesh.shape["parts"], EXPERTS, mesh.shape["expert"] // (2 * EXPERTS), 2, mesh.shape["tensor"]
        ),
        ("parts", "seg", "pos", "core", "tensor"),
    )
    return jax.shard_map(
        on_device,
        mesh=split,
        in_specs=(
            P(PARTS_EXPERT, "tensor"),
            P(PARTS_EXPERT, "tensor", None),
            P(None, PARTS_EXPERT, "tensor", None),
            P(None, PARTS_EXPERT, None, "tensor", None),
            P(PARTS_EXPERT),
            P("tensor"),
            P("tensor", EXPERT),
            P("tensor", EXPERT),
            P(EXPERT, "tensor"),
            P(PARTS_EXPERT, None),
            P(PARTS_EXPERT, None),
        ),
        out_specs=P(PARTS_EXPERT, "tensor"),
        check_vma=False,
    )
```

```python
import functools
import math

import jax
import jax.numpy as jnp
from jax import lax
from jax.experimental import pallas as pl
from jax.experimental.pallas import tpu as pltpu
from jax.sharding import Mesh
from jax.sharding import PartitionSpec as P


EXPERTS = 4
CAP = 9
EXPERT = ("seg", "pos", "core")
PARTS_EXPERT = ("parts", "seg", "pos", "core")
LANES = 128

EPSILON = 1e-05


def from_partner(x, axis, apart):
    return lax.ppermute(x, axis, [(i, i ^ apart) for i in range(lax.axis_size(axis))])


def attend(queries, new_kv, cache_kv, lengths):
    sequences, head_count, head_size = queries.shape
    key_heads = new_kv.shape[2]
    groups = head_count // key_heads
    factor = 1.0 / math.sqrt(head_size)
    query_grp = queries.reshape(sequences, key_heads, groups, head_size)
    score_old = (
        jnp.einsum("skgd,spkd->skgp", query_grp, cache_kv[0], preferred_element_type=jnp.float32)
        * factor
    )
    score_new = (
        jnp.einsum("skgd,skd->skg", query_grp, new_kv[0], preferred_element_type=jnp.float32)
        * factor
    )
    position = jnp.arange(cache_kv.shape[2], dtype=jnp.int32)
    usable = (position[None, :] < lengths[:, None])[:, None, None, :]
    score_old = jnp.where(usable, score_old, -jnp.inf)
    largest = jnp.maximum(jnp.max(score_old, axis=3), score_new)
    weight_old = jnp.exp(score_old - largest[..., None])
    weight_new = jnp.exp(score_new - largest)
    denominator = jnp.sum(weight_old, axis=3) + weight_new
    prob_old = (weight_old / denominator[..., None]).astype(jnp.bfloat16)
    prob_new = (weight_new / denominator).astype(jnp.bfloat16)
    attended = jnp.einsum(
        "skgp,spkd->skgd", prob_old, cache_kv[1], preferred_element_type=jnp.float32
    )
    attended = (
        attended
        + prob_new.astype(jnp.float32)[..., None] * new_kv[1].astype(jnp.float32)[:, :, None, :]
    )
    return attended.reshape(sequences, head_count * head_size)


def between_segments(blocks):
    segs, places, cores = (lax.axis_size(a) for a in EXPERT)
    groups = [
        [
            (seg * places + (place + places // 2 * (2 * seg // segs)) % places) * cores + core
            for seg in range(segs)
        ]
        for place in range(places)
        for core in range(cores)
    ]
    return lax.all_to_all(
        blocks, EXPERT, split_axis=0, concat_axis=0, tiled=True, axis_index_groups=groups
    )


def kept(x):
    return pltpu.with_memory_space_constraint(x, pltpu.VMEM)


def up_kernel(*refs):
    pieces, (gain_ref, gate_ref, up_ref, out_ref, rows_ref) = refs[:-5], refs[-5:]
    across, share, _ = out_ref.shape
    columns = gate_ref.shape[1]
    count = pieces[0].shape[0]
    inverse = 1.0 / gain_ref[...]
    lane = lax.broadcasted_iota(jnp.int32, (count, LANES), 1)
    for i, piece in enumerate(pieces):
        rows = piece[...]
        rows_ref[i * count : (i + 1) * count, :] = rows
        plain = rows.astype(jnp.float32) * inverse
        squares = jnp.sum(plain * plain, axis=1, keepdims=True)
        high = squares.astype(jnp.bfloat16).astype(jnp.float32)
        both = jnp.where(lane == 0, high, squares - high).astype(jnp.bfloat16)
        out_ref[i, :, 2 * columns :] = both
    for at, weight in ((0, gate_ref), (columns, up_ref)):
        sums = jnp.dot(rows_ref[...], weight[...], preferred_element_type=jnp.float32)
        sums = sums.astype(jnp.bfloat16)
        for i in range(across):
            out_ref[i, :, at : at + columns] = sums[i * share : (i + 1) * share]


def up_part(pieces, gain, gate_weight, up_weight):
    count, local_width = pieces[0].shape
    columns = gate_weight.shape[1]
    across = lax.axis_size("tensor")
    assert across == len(pieces)
    whole = pl.BlockSpec(memory_space=pltpu.VMEM)
    return pl.pallas_call(
        up_kernel,
        out_shape=pltpu.VMEM((across, count, 2 * columns + LANES), jnp.bfloat16),
        in_specs=[whole] * (len(pieces) + 3),
        out_specs=whole,
        scratch_shapes=[pltpu.VMEM((len(pieces) * count, local_width), jnp.bfloat16)],
        compiler_params=pltpu.CompilerParams(vmem_limit_bytes=16 << 20),
        name="up",
    )(*map(kept, (*pieces, gain.reshape(1, local_width), gate_weight, up_weight)))


def hidden_kernel(full_width, sums_ref, out_ref):
    across, _, width = sums_ref.shape
    columns = (width - LANES) // 2
    total = sums_ref[0].astype(jnp.float32)
    for i in range(1, across):
        total = total + sums_ref[i].astype(jnp.float32)
    squares = total[:, 2 * columns : 2 * columns + 1] + total[:, 2 * columns + 1 : 2 * columns + 2]
    scale = lax.rsqrt(squares / full_width + EPSILON)
    gate = total[:, :columns] * scale
    lift = total[:, columns : 2 * columns] * scale
    hidden = (gate / (1.0 + jnp.exp(-gate)) * lift).astype(jnp.bfloat16)
    for i in range(across):
        out_ref[i] = hidden


def activated(sums, full_width):
    across, count, width = sums.shape
    whole = pl.BlockSpec(memory_space=pltpu.VMEM)
    return pl.pallas_call(
        functools.partial(hidden_kernel, full_width),
        out_shape=pltpu.VMEM((across, count, (width - LANES) // 2), jnp.bfloat16),
        in_specs=[whole],
        out_specs=whole,
        compiler_params=pltpu.CompilerParams(vmem_limit_bytes=8 << 20),
        name="hidden",
    )(kept(sums))


def send(x):
    return x.astype(jnp.bfloat16)


def gathered(own):
    by4 = from_partner(own, "pos", 4)
    by2 = from_partner(own, "pos", 2)
    by6 = from_partner(by4, "pos", 2)
    near = jnp.concatenate([own, by4], axis=0)
    far = jnp.concatenate([by2, by6], axis=0)
    near_next = from_partner(near, "pos", 1)
    far_next = from_partner(far, "pos", 1)
    held = jnp.concatenate([near, far], axis=0)
    held_there = from_partner(held, "core", 1)
    following = jnp.concatenate([near_next, far_next], axis=0)
    following_there = from_partner(following, "core", 1)
    return held, following, held_there, following_there


def down_kernel(hidden_ref, weight_ref, *outs):
    count = hidden_ref.shape[1]
    hidden = hidden_ref[...].reshape(-1, hidden_ref.shape[2])
    width = weight_ref.shape[1] // 3
    for start in range(0, 3 * width, width):
        columns = slice(start, start + width)
        terms = jnp.dot(hidden, weight_ref[:, columns], preferred_element_type=jnp.float32)
        for i, out in enumerate(outs):
            out[:, columns] = terms[i * count : (i + 1) * count].astype(out.dtype)


def down_part(hidden, down_weight):
    _, count, _ = hidden.shape
    width = down_weight.shape[1]
    whole = pl.BlockSpec(memory_space=pltpu.VMEM)
    kinds = (jnp.float32, jnp.float32, jnp.bfloat16, jnp.bfloat16)
    return pl.pallas_call(
        down_kernel,
        out_shape=[pltpu.VMEM((count, width), kind) for kind in kinds],
        in_specs=[whole, whole],
        out_specs=[whole] * len(kinds),
        compiler_params=pltpu.CompilerParams(vmem_limit_bytes=16 << 20),
        name="down",
    )(kept(hidden), kept(down_weight))


def summed(held, following, held_there, following_there):
    half = held.shape[0] // 2
    own = half // 2
    here = from_partner(following_there, "core", 1).astype(jnp.float32)
    following = send(following + here)
    held = held + from_partner(held_there, "core", 1).astype(jnp.float32)
    near, far = lax.optimization_barrier((held[:half], held[half:]))
    far = far + from_partner(following[half:], "pos", 1).astype(jnp.float32)
    near = near + from_partner(following[:half], "pos", 1).astype(jnp.float32)
    far = send(far)
    by4 = near[own:] + from_partner(far[own:], "pos", 2).astype(jnp.float32)
    home = near[:own] + from_partner(far[:own], "pos", 2).astype(jnp.float32)
    return home + from_partner(send(by4), "pos", 4).astype(jnp.float32)


def through_expert(pieces, gain, gate_weight, up_weight, down_weight):
    across = lax.axis_size("tensor")
    sums = up_part(pieces, gain, gate_weight, up_weight)
    sums = lax.all_to_all(sums, "tensor", split_axis=0, concat_axis=0, tiled=True)
    copies = activated(sums, gate_weight.shape[0] * across)
    hidden = lax.all_to_all(copies, "tensor", split_axis=0, concat_axis=0, tiled=True)
    return down_part(hidden, down_weight)


def on_device(
    tokens,
    queries,
    new_kv,
    cache_kv,
    lengths,
    gain,
    gate_weight,
    up_weight,
    down_weight,
    routes,
    route_weights,
):
    local_seqs, local_width = tokens.shape
    residual = tokens.astype(jnp.float32) + attend(queries, new_kv, cache_kv, lengths)
    scaled = (residual * gain).astype(jnp.bfloat16)
    choosers = (routes[:, :, None] == jnp.arange(EXPERTS, dtype=jnp.int32)[None, None, :]).astype(
        jnp.int32
    )
    flat_choice = choosers.reshape(2 * local_seqs, EXPERTS)
    earlier = jnp.cumsum(flat_choice, axis=0) - flat_choice
    slot_index = jnp.sum(earlier * flat_choice, axis=1)
    target = (routes.reshape(-1) * CAP + slot_index).reshape(local_seqs, 2)
    slot_ids = jnp.arange(EXPERTS * CAP, dtype=jnp.int32)
    placing = jnp.sum(
        (slot_ids[:, None, None] == target[None, :, :]).astype(jnp.float32), axis=2
    ).astype(jnp.bfloat16)
    mixing = jnp.sum(
        jnp.where(
            slot_ids[None, None, :] == target[:, :, None],
            route_weights.astype(jnp.float32)[:, :, None],
            jnp.float32(0.0),
        ),
        axis=1,
    ).astype(jnp.bfloat16)
    packed = jnp.dot(placing, scaled, preferred_element_type=jnp.float32).astype(jnp.bfloat16)
    flat = packed.reshape(EXPERTS, CAP * local_width // LANES, LANES)
    rows = between_segments(flat).reshape(EXPERTS * CAP, local_width)
    terms = through_expert(gathered(rows), gain, gate_weight, up_weight, down_weight)
    results = summed(*terms).astype(jnp.bfloat16)
    results, mixing = lax.optimization_barrier((results, mixing))
    per_slot = between_segments(results.reshape(flat.shape)).reshape(EXPERTS * CAP, local_width)
    moe_sum = jnp.dot(mixing, per_slot, preferred_element_type=jnp.float32)
    return (residual + moe_sum).astype(jnp.bfloat16)


def solution(mesh):
    split = Mesh(
        mesh.devices.reshape(
            mesh.shape["parts"], EXPERTS, mesh.shape["expert"] // (2 * EXPERTS), 2, mesh.shape["tensor"]
        ),
        ("parts", "seg", "pos", "core", "tensor"),
    )
    return jax.shard_map(
        on_device,
        mesh=split,
        in_specs=(
            P(PARTS_EXPERT, "tensor"),
            P(PARTS_EXPERT, "tensor", None),
            P(None, PARTS_EXPERT, "tensor", None),
            P(None, PARTS_EXPERT, None, "tensor", None),
            P(PARTS_EXPERT),
            P("tensor"),
            P("tensor", EXPERT),
            P("tensor", EXPERT),
            P(EXPERT, "tensor"),
            P(PARTS_EXPERT, None),
            P(PARTS_EXPERT, None),
        ),
        out_specs=P(PARTS_EXPERT, "tensor"),
        check_vma=False,
    )
```

```python
import functools
import math

import jax
import jax.numpy as jnp
from jax import lax
from jax.experimental import pallas as pl
from jax.experimental.pallas import tpu as pltpu
from jax.sharding import Mesh
from jax.sharding import PartitionSpec as P


EXPERTS = 4
CAP = 9
EXPERT = ("seg", "pos", "core")
PARTS_EXPERT = ("parts", "seg", "pos", "core")
LANES = 128

EPSILON = 1e-05


def from_partner(x, axis, apart):
    return lax.ppermute(x, axis, [(i, i ^ apart) for i in range(lax.axis_size(axis))])


def pack_kernel(*refs):
    sources, (residual_ref, packed_ref, mixing_ref) = refs[:8], refs[8:11]
    rows_ref, here, arrived = refs[11], refs[12:20], refs[20]
    copies = [
        pltpu.make_async_copy(source, target, arrived.at[i])
        for i, (source, target) in enumerate(zip(sources, here))
    ]
    for copy in copies:
        copy.start()
    for copy in copies:
        copy.wait()
    cache_ref, queries_ref, new_ref, tokens_ref, gain_ref, lengths_ref, routes_ref, weights_ref = here
    count, head_size = queries_ref.shape
    sequences, _ = tokens_ref.shape
    heads = count // sequences
    key_heads = new_ref.shape[1] // sequences
    cached = cache_ref.shape[1]
    places = cached // (sequences * key_heads)
    group = heads // key_heads
    factor = 1.0 / math.sqrt(head_size)

    def matching(shape, per_sequence):
        row = lax.broadcasted_iota(jnp.int32, shape, 0)
        column = lax.broadcasted_iota(jnp.int32, shape, 1)
        same = row % sequences == column // per_sequence
        return same & (row // (sequences * group) == column % key_heads)

    queries = queries_ref[...]
    across = (((1,), (1,)), ((), ()))
    old = lax.dot_general(queries, cache_ref[0], across, preferred_element_type=jnp.float32) * factor
    new = lax.dot_general(queries, new_ref[0], across, preferred_element_type=jnp.float32) * factor
    limit = jnp.zeros((1, cached), jnp.int32)
    column = lax.broadcasted_iota(jnp.int32, (1, cached), 1)
    for i in range(sequences):
        limit = jnp.where(column // (places * key_heads) == i, lengths_ref[i], limit)
    usable = column // key_heads % places < limit
    old = jnp.where(matching(old.shape, places * key_heads) & usable, old, -jnp.inf)
    new = jnp.where(matching(new.shape, key_heads), new, -jnp.inf)
    largest = jnp.maximum(jnp.max(old, axis=1, keepdims=True), jnp.max(new, axis=1, keepdims=True))
    old = jnp.exp(old - largest)
    new = jnp.exp(new - largest)
    total = jnp.sum(old, axis=1, keepdims=True) + jnp.sum(new, axis=1, keepdims=True)
    old = (old / total).astype(jnp.bfloat16)
    new = (new / total).astype(jnp.bfloat16)
    rows_ref[...] = jnp.dot(old, cache_ref[1], preferred_element_type=jnp.float32) + jnp.dot(
        new, new_ref[1], preferred_element_type=jnp.float32
    )
    slots = packed_ref.shape[0]
    slot = lax.broadcasted_iota(jnp.int32, (slots, sequences), 0)
    column = lax.broadcasted_iota(jnp.int32, (1, sequences), 1)
    targets = [jnp.zeros((1, sequences), jnp.int32) for _ in range(2)]
    used = [jnp.int32(0)] * EXPERTS
    for i in range(sequences):
        for j in range(2):
            route = routes_ref[j, i]
            target = jnp.int32(0)
            for k in range(EXPERTS):
                target = jnp.where(route == k, k * CAP + used[k], target)
                used[k] = used[k] + jnp.where(route == k, 1, 0)
            targets[j] = jnp.where(column == i, target, targets[j])
    weights = weights_ref[...].astype(jnp.float32)
    mixing = jnp.where(slot == targets[0], weights[0:1], 0.0)
    mixing_ref[...] = jnp.where(slot == targets[1], weights[1:2], mixing).astype(jnp.bfloat16)
    placing = jnp.where((slot == targets[0]) | (slot == targets[1]), 1.0, 0.0).astype(jnp.bfloat16)
    for h in range(heads):
        at = slice(h * head_size, (h + 1) * head_size)
        attended = rows_ref[h * sequences : (h + 1) * sequences, :]
        residual = tokens_ref[:, at].astype(jnp.float32) + attended
        residual_ref[:, at] = residual
        scaled = (residual * gain_ref[h : h + 1]).astype(jnp.bfloat16)
        packed = jnp.dot(placing, scaled, preferred_element_type=jnp.float32)
        packed_ref[:, at] = packed.astype(jnp.bfloat16)


def pack_part(tokens, queries, new_kv, cache_kv, lengths, gain, routes, route_weights):
    sequences, width = tokens.shape
    _, heads, head_size = queries.shape
    slots = EXPERTS * CAP
    whole = pl.BlockSpec(memory_space=pltpu.VMEM)
    arrays = (
        cache_kv.reshape(2, -1, head_size),
        queries.transpose(1, 0, 2).reshape(heads * sequences, head_size),
        new_kv.reshape(2, -1, head_size),
        tokens,
        gain.reshape(heads, head_size),
        lengths,
        routes.T,
        route_weights.T,
    )
    places = [pltpu.SMEM if a.dtype == jnp.int32 else pltpu.VMEM for a in arrays]
    return pl.pallas_call(
        pack_kernel,
        out_shape=[
            pltpu.VMEM((sequences, width), jnp.float32),
            pltpu.VMEM((slots, width), jnp.bfloat16),
            pltpu.VMEM((slots, sequences), jnp.bfloat16),
        ],
        in_specs=[pl.BlockSpec(memory_space=pltpu.HBM)] * len(arrays),
        out_specs=[whole] * 3,
        scratch_shapes=[
            pltpu.VMEM((sequences * heads, head_size), jnp.float32),
            *(place(a.shape, a.dtype) for place, a in zip(places, arrays)),
            pltpu.SemaphoreType.DMA((len(arrays),)),
        ],
        compiler_params=pltpu.CompilerParams(vmem_limit_bytes=16 << 20),
        name="pack",
    )(*(pltpu.with_memory_space_constraint(a, pltpu.HBM) for a in arrays))


def between_segments(blocks):
    segs, places, cores = (lax.axis_size(a) for a in EXPERT)
    groups = [
        [
            (seg * places + (place + places // 2 * (2 * seg // segs)) % places) * cores + core
            for seg in range(segs)
        ]
        for place in range(places)
        for core in range(cores)
    ]
    return lax.all_to_all(
        blocks, EXPERT, split_axis=0, concat_axis=0, tiled=True, axis_index_groups=groups
    )


def kept(x):
    return pltpu.with_memory_space_constraint(x, pltpu.VMEM)


def up_kernel(*refs):
    pieces, (gain_ref, gate_ref, up_ref, out_ref, rows_ref) = refs[:-5], refs[-5:]
    across, share, _ = out_ref.shape
    columns = gate_ref.shape[1]
    count = pieces[0].shape[0]
    inverse = 1.0 / gain_ref[...]
    lane = lax.broadcasted_iota(jnp.int32, (count, LANES), 1)
    for i, piece in enumerate(pieces):
        rows = piece[...]
        rows_ref[i * count : (i + 1) * count, :] = rows
        squares = jnp.zeros((count, LANES), jnp.float32)
        for c in range(inverse.shape[0]):
            plain = rows[:, c * LANES : (c + 1) * LANES].astype(jnp.float32) * inverse[c : c + 1]
            squares = squares + plain * plain
        squares = jnp.sum(squares, axis=1, keepdims=True)
        high = squares.astype(jnp.bfloat16).astype(jnp.float32)
        both = jnp.where(lane == 0, high, squares - high).astype(jnp.bfloat16)
        out_ref[i, :, 2 * columns :] = both
    for at, weight in ((0, gate_ref), (columns, up_ref)):
        sums = jnp.dot(rows_ref[...], weight[...], preferred_element_type=jnp.float32)
        sums = sums.astype(jnp.bfloat16)
        for i in range(across):
            out_ref[i, :, at : at + columns] = sums[i * share : (i + 1) * share]


def up_part(pieces, gain, gate_weight, up_weight):
    count, local_width = pieces[0].shape
    columns = gate_weight.shape[1]
    across = lax.axis_size("tensor")
    assert across == len(pieces)
    whole = pl.BlockSpec(memory_space=pltpu.VMEM)
    return pl.pallas_call(
        up_kernel,
        out_shape=pltpu.VMEM((across, count, 2 * columns + LANES), jnp.bfloat16),
        in_specs=[whole] * (len(pieces) + 3),
        out_specs=whole,
        scratch_shapes=[pltpu.VMEM((len(pieces) * count, local_width), jnp.bfloat16)],
        compiler_params=pltpu.CompilerParams(vmem_limit_bytes=16 << 20),
        name="up",
    )(*map(kept, (*pieces, gain.reshape(-1, LANES), gate_weight, up_weight)))


def hidden_kernel(full_width, sums_ref, out_ref):
    across, _, width = sums_ref.shape
    columns = (width - LANES) // 2
    total = sums_ref[0].astype(jnp.float32)
    for i in range(1, across):
        total = total + sums_ref[i].astype(jnp.float32)
    squares = total[:, 2 * columns : 2 * columns + 1] + total[:, 2 * columns + 1 : 2 * columns + 2]
    scale = lax.rsqrt(squares / full_width + EPSILON)
    gate = total[:, :columns] * scale
    lift = total[:, columns : 2 * columns] * scale
    hidden = (gate / (1.0 + jnp.exp(-gate)) * lift).astype(jnp.bfloat16)
    for i in range(across):
        out_ref[i] = hidden


def activated(sums, full_width):
    across, count, width = sums.shape
    whole = pl.BlockSpec(memory_space=pltpu.VMEM)
    return pl.pallas_call(
        functools.partial(hidden_kernel, full_width),
        out_shape=pltpu.VMEM((across, count, (width - LANES) // 2), jnp.bfloat16),
        in_specs=[whole],
        out_specs=whole,
        compiler_params=pltpu.CompilerParams(vmem_limit_bytes=8 << 20),
        name="hidden",
    )(kept(sums))


def send(x):
    return x.astype(jnp.bfloat16)


def gathered(own):
    by4 = from_partner(own, "pos", 4)
    by2 = from_partner(own, "pos", 2)
    by6 = from_partner(by4, "pos", 2)
    near = jnp.concatenate([own, by4], axis=0)
    far = jnp.concatenate([by2, by6], axis=0)
    near_next = from_partner(near, "pos", 1)
    far_next = from_partner(far, "pos", 1)
    held = jnp.concatenate([near, far], axis=0)
    held_there = from_partner(held, "core", 1)
    following = jnp.concatenate([near_next, far_next], axis=0)
    following_there = from_partner(following, "core", 1)
    return held, following, held_there, following_there


def down_kernel(hidden_ref, weight_ref, *outs):
    count = hidden_ref.shape[1]
    hidden = hidden_ref[...].reshape(-1, hidden_ref.shape[2])
    width = weight_ref.shape[1] // 3
    for start in range(0, 3 * width, width):
        columns = slice(start, start + width)
        terms = jnp.dot(hidden, weight_ref[:, columns], preferred_element_type=jnp.float32)
        for i, out in enumerate(outs):
            out[:, columns] = terms[i * count : (i + 1) * count].astype(out.dtype)


def down_part(hidden, down_weight):
    _, count, _ = hidden.shape
    width = down_weight.shape[1]
    whole = pl.BlockSpec(memory_space=pltpu.VMEM)
    kinds = (jnp.float32, jnp.float32, jnp.bfloat16, jnp.bfloat16)
    return pl.pallas_call(
        down_kernel,
        out_shape=[pltpu.VMEM((count, width), kind) for kind in kinds],
        in_specs=[whole, whole],
        out_specs=[whole] * len(kinds),
        compiler_params=pltpu.CompilerParams(vmem_limit_bytes=16 << 20),
        name="down",
    )(kept(hidden), kept(down_weight))


def summed(held, following, held_there, following_there):
    half = held.shape[0] // 2
    own = half // 2
    here = from_partner(following_there, "core", 1).astype(jnp.float32)
    following = send(following + here)
    held = held + from_partner(held_there, "core", 1).astype(jnp.float32)
    near, far = lax.optimization_barrier((held[:half], held[half:]))
    far = far + from_partner(following[half:], "pos", 1).astype(jnp.float32)
    near = near + from_partner(following[:half], "pos", 1).astype(jnp.float32)
    far = send(far)
    by4 = near[own:] + from_partner(far[own:], "pos", 2).astype(jnp.float32)
    home = near[:own] + from_partner(far[:own], "pos", 2).astype(jnp.float32)
    return home + from_partner(send(by4), "pos", 4).astype(jnp.float32)


def through_expert(pieces, gain, gate_weight, up_weight, down_weight):
    across = lax.axis_size("tensor")
    sums = up_part(pieces, gain, gate_weight, up_weight)
    sums = lax.all_to_all(sums, "tensor", split_axis=0, concat_axis=0, tiled=True)
    copies = activated(sums, gate_weight.shape[0] * across)
    hidden = lax.all_to_all(copies, "tensor", split_axis=0, concat_axis=0, tiled=True)
    return down_part(hidden, down_weight)


def on_device(
    tokens,
    queries,
    new_kv,
    cache_kv,
    lengths,
    gain,
    gate_weight,
    up_weight,
    down_weight,
    routes,
    route_weights,
):
    _, local_width = tokens.shape
    residual, packed, mixing = pack_part(
        tokens, queries, new_kv, cache_kv, lengths, gain, routes, route_weights
    )
    flat = packed.reshape(EXPERTS, CAP * local_width // LANES, LANES)
    rows = between_segments(flat).reshape(EXPERTS * CAP, local_width)
    terms = through_expert(gathered(rows), gain, gate_weight, up_weight, down_weight)
    results = summed(*terms).astype(jnp.bfloat16)
    per_slot = between_segments(results.reshape(flat.shape)).reshape(EXPERTS * CAP, local_width)
    moe_sum = lax.dot_general(
        mixing, per_slot, (((0,), (0,)), ((), ())), preferred_element_type=jnp.float32
    )
    return (residual + moe_sum).astype(jnp.bfloat16)


def solution(mesh):
    split = Mesh(
        mesh.devices.reshape(
            mesh.shape["parts"], EXPERTS, mesh.shape["expert"] // (2 * EXPERTS), 2, mesh.shape["tensor"]
        ),
        ("parts", "seg", "pos", "core", "tensor"),
    )
    return jax.shard_map(
        on_device,
        mesh=split,
        in_specs=(
            P(PARTS_EXPERT, "tensor"),
            P(PARTS_EXPERT, "tensor", None),
            P(None, PARTS_EXPERT, "tensor", None),
            P(None, PARTS_EXPERT, None, "tensor", None),
            P(PARTS_EXPERT),
            P("tensor"),
            P("tensor", EXPERT),
            P("tensor", EXPERT),
            P(EXPERT, "tensor"),
            P(PARTS_EXPERT, None),
            P(PARTS_EXPERT, None),
        ),
        out_specs=P(PARTS_EXPERT, "tensor"),
        check_vma=False,
    )
```

```python
import functools
import math

import jax
import jax.numpy as jnp
from jax import lax
from jax.experimental import pallas as pl
from jax.experimental.pallas import tpu as pltpu
from jax.sharding import Mesh
from jax.sharding import PartitionSpec as P


EXPERTS = 4
CAP = 9
EXPERT = ("seg", "pos", "core")
PARTS_EXPERT = ("parts", "seg", "pos", "core")
LANES = 128

EPSILON = 1e-05


def from_partner(x, axis, apart):
    return lax.ppermute(x, axis, [(i, i ^ apart) for i in range(lax.axis_size(axis))])


def pack_kernel(*refs):
    sources, (residual_ref, packed_ref, mixing_ref) = refs[:8], refs[8:11]
    rows_ref, here, arrived = refs[11], refs[12:20], refs[20]
    copies = [
        pltpu.make_async_copy(source, target, arrived.at[i])
        for i, (source, target) in enumerate(zip(sources, here))
    ]
    for copy in copies:
        copy.start()
    for copy in copies:
        copy.wait()
    cache_ref, queries_ref, new_ref, tokens_ref, gain_ref, lengths_ref, routes_ref, weights_ref = here
    count, head_size = queries_ref.shape
    sequences, _ = tokens_ref.shape
    heads = count // sequences
    key_heads = new_ref.shape[1] // sequences
    cached = cache_ref.shape[1]
    places = cached // (sequences * key_heads)
    group = heads // key_heads
    factor = 1.0 / math.sqrt(head_size)

    def matching(shape, per_sequence):
        row = lax.broadcasted_iota(jnp.int32, shape, 0)
        column = lax.broadcasted_iota(jnp.int32, shape, 1)
        same = row % sequences == column // per_sequence
        return same & (row // (sequences * group) == column % key_heads)

    queries = queries_ref[...]
    across = (((1,), (1,)), ((), ()))
    old = lax.dot_general(queries, cache_ref[0], across, preferred_element_type=jnp.float32) * factor
    new = lax.dot_general(queries, new_ref[0], across, preferred_element_type=jnp.float32) * factor
    limit = jnp.zeros((1, cached), jnp.int32)
    column = lax.broadcasted_iota(jnp.int32, (1, cached), 1)
    for i in range(sequences):
        limit = jnp.where(column // (places * key_heads) == i, lengths_ref[i], limit)
    usable = column // key_heads % places < limit
    old = jnp.where(matching(old.shape, places * key_heads) & usable, old, -jnp.inf)
    new = jnp.where(matching(new.shape, key_heads), new, -jnp.inf)
    largest = jnp.maximum(jnp.max(old, axis=1, keepdims=True), jnp.max(new, axis=1, keepdims=True))
    old = jnp.exp(old - largest)
    new = jnp.exp(new - largest)
    total = jnp.sum(old, axis=1, keepdims=True) + jnp.sum(new, axis=1, keepdims=True)
    old = (old / total).astype(jnp.bfloat16)
    new = (new / total).astype(jnp.bfloat16)
    rows_ref[...] = jnp.dot(old, cache_ref[1], preferred_element_type=jnp.float32) + jnp.dot(
        new, new_ref[1], preferred_element_type=jnp.float32
    )
    slots = packed_ref.shape[0]
    slot = lax.broadcasted_iota(jnp.int32, (slots, sequences), 0)
    column = lax.broadcasted_iota(jnp.int32, (1, sequences), 1)
    targets = [jnp.zeros((1, sequences), jnp.int32) for _ in range(2)]
    used = [jnp.int32(0)] * EXPERTS
    for i in range(sequences):
        for j in range(2):
            route = routes_ref[j, i]
            target = jnp.int32(0)
            for k in range(EXPERTS):
                target = jnp.where(route == k, k * CAP + used[k], target)
                used[k] = used[k] + jnp.where(route == k, 1, 0)
            targets[j] = jnp.where(column == i, target, targets[j])
    weights = weights_ref[...].astype(jnp.float32)
    mixing = jnp.where(slot == targets[0], weights[0:1], 0.0)
    mixing_ref[...] = jnp.where(slot == targets[1], weights[1:2], mixing).astype(jnp.bfloat16)
    placing = jnp.where((slot == targets[0]) | (slot == targets[1]), 1.0, 0.0).astype(jnp.bfloat16)
    for h in range(heads):
        at = slice(h * head_size, (h + 1) * head_size)
        attended = rows_ref[h * sequences : (h + 1) * sequences, :]
        residual = tokens_ref[:, at].astype(jnp.float32) + attended
        residual_ref[:, at] = residual
        scaled = (residual * gain_ref[h : h + 1]).astype(jnp.bfloat16)
        packed = jnp.dot(placing, scaled, preferred_element_type=jnp.float32)
        packed_ref[:, at] = packed.astype(jnp.bfloat16)


def pack_part(tokens, queries, new_kv, cache_kv, lengths, gain, routes, route_weights):
    sequences, width = tokens.shape
    _, heads, head_size = queries.shape
    slots = EXPERTS * CAP
    whole = pl.BlockSpec(memory_space=pltpu.VMEM)
    arrays = (
        cache_kv.reshape(2, -1, head_size),
        queries.transpose(1, 0, 2).reshape(heads * sequences, head_size),
        new_kv.reshape(2, -1, head_size),
        tokens,
        gain.reshape(heads, head_size),
        lengths,
        routes.T,
        route_weights.T,
    )
    places = [pltpu.SMEM if a.dtype == jnp.int32 else pltpu.VMEM for a in arrays]
    return pl.pallas_call(
        pack_kernel,
        out_shape=[
            pltpu.VMEM((sequences, width), jnp.float32),
            pltpu.VMEM((slots, width), jnp.bfloat16),
            pltpu.VMEM((slots, sequences), jnp.bfloat16),
        ],
        in_specs=[pl.BlockSpec(memory_space=pltpu.HBM)] * len(arrays),
        out_specs=[whole] * 3,
        scratch_shapes=[
            pltpu.VMEM((sequences * heads, head_size), jnp.float32),
            *(place(a.shape, a.dtype) for place, a in zip(places, arrays)),
            pltpu.SemaphoreType.DMA((len(arrays),)),
        ],
        compiler_params=pltpu.CompilerParams(vmem_limit_bytes=16 << 20),
        name="pack",
    )(*(pltpu.with_memory_space_constraint(a, pltpu.HBM) for a in arrays))


def between_segments(blocks):
    segs, places, cores = (lax.axis_size(a) for a in EXPERT)
    groups = [
        [
            (seg * places + (place + places // 2 * (2 * seg // segs)) % places) * cores + core
            for seg in range(segs)
        ]
        for place in range(places)
        for core in range(cores)
    ]
    return lax.all_to_all(
        blocks, EXPERT, split_axis=0, concat_axis=0, tiled=True, axis_index_groups=groups
    )


def kept(x):
    return pltpu.with_memory_space_constraint(x, pltpu.VMEM)


def up_kernel(*refs):
    pieces, (gain_ref, gate_ref, up_ref, out_ref, rows_ref) = refs[:-5], refs[-5:]
    across, share = out_ref.shape[0], out_ref.shape[1] // 2
    columns = gate_ref.shape[1]
    count = pieces[0].shape[0]
    inverse = 1.0 / gain_ref[...]
    lane = lax.broadcasted_iota(jnp.int32, (count, LANES), 1)
    for i, piece in enumerate(pieces):
        rows = piece[...]
        rows_ref[i * count : (i + 1) * count, :] = rows
        squares = jnp.zeros((count, LANES), jnp.float32)
        for c in range(inverse.shape[0]):
            plain = rows[:, c * LANES : (c + 1) * LANES].astype(jnp.float32) * inverse[c : c + 1]
            squares = squares + plain * plain
        squares = jnp.sum(squares, axis=1, keepdims=True)
        high = squares.astype(jnp.bfloat16).astype(jnp.float32)
        both = jnp.where(lane == 0, high, squares - high).astype(jnp.bfloat16)
        out_ref[i, :share, columns:] = both
        out_ref[i, share:, columns:] = jnp.zeros_like(both)
    for at, weight in ((0, gate_ref), (share, up_ref)):
        sums = jnp.dot(rows_ref[...], weight[...], preferred_element_type=jnp.float32)
        sums = sums.astype(jnp.bfloat16)
        for i in range(across):
            out_ref[i, at : at + share, :columns] = sums[i * share : (i + 1) * share]


def up_part(pieces, gain, gate_weight, up_weight):
    count, local_width = pieces[0].shape
    columns = gate_weight.shape[1]
    across = lax.axis_size("tensor")
    assert across == len(pieces)
    whole = pl.BlockSpec(memory_space=pltpu.VMEM)
    return pl.pallas_call(
        up_kernel,
        out_shape=pltpu.VMEM((across, 2 * count, columns + LANES), jnp.bfloat16),
        in_specs=[whole] * (len(pieces) + 3),
        out_specs=whole,
        scratch_shapes=[pltpu.VMEM((len(pieces) * count, local_width), jnp.bfloat16)],
        compiler_params=pltpu.CompilerParams(vmem_limit_bytes=16 << 20),
        name="up",
    )(*map(kept, (*pieces, gain.reshape(-1, LANES), gate_weight, up_weight)))


def hidden_kernel(full_width, sums_ref, out_ref):
    across, count, columns = out_ref.shape
    total = sums_ref[0].astype(jnp.float32)
    for i in range(1, across):
        total = total + sums_ref[i].astype(jnp.float32)
    squares = total[:count, columns : columns + 1] + total[:count, columns + 1 : columns + 2]
    scale = lax.rsqrt(squares / full_width + EPSILON)
    gate = total[:count, :columns] * scale
    lift = total[count:, :columns] * scale
    hidden = (gate / (1.0 + jnp.exp(-gate)) * lift).astype(jnp.bfloat16)
    for i in range(across):
        out_ref[i] = hidden


def activated(sums, full_width):
    across, count, width = sums.shape
    whole = pl.BlockSpec(memory_space=pltpu.VMEM)
    return pl.pallas_call(
        functools.partial(hidden_kernel, full_width),
        out_shape=pltpu.VMEM((across, count // 2, width - LANES), jnp.bfloat16),
        in_specs=[whole],
        out_specs=whole,
        compiler_params=pltpu.CompilerParams(vmem_limit_bytes=8 << 20),
        name="hidden",
    )(kept(sums))


def send(x):
    return x.astype(jnp.bfloat16)


def gathered(own):
    by4 = from_partner(own, "pos", 4)
    by2 = from_partner(own, "pos", 2)
    by6 = from_partner(by4, "pos", 2)
    near = jnp.concatenate([own, by4], axis=0)
    far = jnp.concatenate([by2, by6], axis=0)
    near_next = from_partner(near, "pos", 1)
    far_next = from_partner(far, "pos", 1)
    held = jnp.concatenate([near, far], axis=0)
    held_there = from_partner(held, "core", 1)
    following = jnp.concatenate([near_next, far_next], axis=0)
    following_there = from_partner(following, "core", 1)
    return held, following, held_there, following_there


def down_kernel(hidden_ref, weight_ref, *outs):
    count = hidden_ref.shape[1]
    hidden = hidden_ref[...].reshape(-1, hidden_ref.shape[2])
    width = weight_ref.shape[1] // 3
    for start in range(0, 3 * width, width):
        columns = slice(start, start + width)
        terms = jnp.dot(hidden, weight_ref[:, columns], preferred_element_type=jnp.float32)
        for i, out in enumerate(outs):
            out[:, columns] = terms[i * count : (i + 1) * count].astype(out.dtype)


def down_part(hidden, down_weight):
    _, count, _ = hidden.shape
    width = down_weight.shape[1]
    whole = pl.BlockSpec(memory_space=pltpu.VMEM)
    kinds = (jnp.float32, jnp.float32, jnp.bfloat16, jnp.bfloat16)
    return pl.pallas_call(
        down_kernel,
        out_shape=[pltpu.VMEM((count, width), kind) for kind in kinds],
        in_specs=[whole, whole],
        out_specs=[whole] * len(kinds),
        compiler_params=pltpu.CompilerParams(vmem_limit_bytes=16 << 20),
        name="down",
    )(kept(hidden), kept(down_weight))


def summed(held, following, held_there, following_there):
    half = held.shape[0] // 2
    own = half // 2
    here = from_partner(following_there, "core", 1).astype(jnp.float32)
    following = send(following + here)
    held = held + from_partner(held_there, "core", 1).astype(jnp.float32)
    near, far = lax.optimization_barrier((held[:half], held[half:]))
    far = far + from_partner(following[half:], "pos", 1).astype(jnp.float32)
    near = near + from_partner(following[:half], "pos", 1).astype(jnp.float32)
    far = send(far)
    by4 = near[own:] + from_partner(far[own:], "pos", 2).astype(jnp.float32)
    home = near[:own] + from_partner(far[:own], "pos", 2).astype(jnp.float32)
    return home + from_partner(send(by4), "pos", 4).astype(jnp.float32)


def through_expert(pieces, gain, gate_weight, up_weight, down_weight):
    across = lax.axis_size("tensor")
    sums = up_part(pieces, gain, gate_weight, up_weight)
    sums = lax.all_to_all(sums, "tensor", split_axis=0, concat_axis=0, tiled=True)
    copies = activated(sums, gate_weight.shape[0] * across)
    hidden = lax.all_to_all(copies, "tensor", split_axis=0, concat_axis=0, tiled=True)
    return down_part(hidden, down_weight)


def on_device(
    tokens,
    queries,
    new_kv,
    cache_kv,
    lengths,
    gain,
    gate_weight,
    up_weight,
    down_weight,
    routes,
    route_weights,
):
    _, local_width = tokens.shape
    residual, packed, mixing = pack_part(
        tokens, queries, new_kv, cache_kv, lengths, gain, routes, route_weights
    )
    flat = packed.reshape(EXPERTS, CAP * local_width // LANES, LANES)
    rows = between_segments(flat).reshape(EXPERTS * CAP, local_width)
    terms = through_expert(gathered(rows), gain, gate_weight, up_weight, down_weight)
    results = summed(*terms).astype(jnp.bfloat16)
    per_slot = between_segments(results.reshape(flat.shape)).reshape(EXPERTS * CAP, local_width)
    moe_sum = lax.dot_general(
        mixing, per_slot, (((0,), (0,)), ((), ())), preferred_element_type=jnp.float32
    )
    return (residual + moe_sum).astype(jnp.bfloat16)


def solution(mesh):
    split = Mesh(
        mesh.devices.reshape(
            mesh.shape["parts"], EXPERTS, mesh.shape["expert"] // (2 * EXPERTS), 2, mesh.shape["tensor"]
        ),
        ("parts", "seg", "pos", "core", "tensor"),
    )
    return jax.shard_map(
        on_device,
        mesh=split,
        in_specs=(
            P(PARTS_EXPERT, "tensor"),
            P(PARTS_EXPERT, "tensor", None),
            P(None, PARTS_EXPERT, "tensor", None),
            P(None, PARTS_EXPERT, None, "tensor", None),
            P(PARTS_EXPERT),
            P("tensor"),
            P("tensor", EXPERT),
            P("tensor", EXPERT),
            P(EXPERT, "tensor"),
            P(PARTS_EXPERT, None),
            P(PARTS_EXPERT, None),
        ),
        out_specs=P(PARTS_EXPERT, "tensor"),
        check_vma=False,
    )
```
